16 devices in a mesh: dp: 2 (over y, z), tp: 8 (over x, core).
Axes of the slice: x: 4, y: 2, z: 1, core: 2. Of those that a mesh axis runs over, the one named last changes fastest.
The devices are a block of a 4x4x8 slice.
Arguments:
- enc_out: bfloat16 [24, 1024, 1024], P('dp', 'tp'), parts along dimension 0
- norm_scale: bfloat16 [1024], replicated
- w_key: bfloat16 [12, 1024, 16, 64], P(None, None, 'tp')
- w_value: bfloat16 [12, 1024, 16, 64], P(None, None, 'tp')
Outputs:
- output 1: bfloat16 [12, 24, 1024, 16, 64], P(None, 'dp', None, 'tp'), parts along dimension 1
- output 2: bfloat16 [12, 24, 1024, 16, 64], P(None, 'dp', None, 'tp'), parts along dimension 1
There are 2 independent parts. The reference program is written for one: setup_inputs(seed, part) draws one part's arguments, and reference() takes and returns one part's arrays. A program takes and returns all parts, laid end to end along the dimension named above; an argument that names none is the same for every part.
All inputs are finite; a program needn't handle non-finite values.
Results may differ from the reference program's by a relative error of at most 0.001.
Values are sent between devices in bfloat16 or wider.
A program may use at most 768 MiB of HBM per device.

```python
import jax
import jax.numpy as jnp
from jax import lax

N_LAYERS = 12
BATCH_SIZE = 12
SEQ_LEN = 1024
D_MODEL = 1024
N_HEADS = 16
HEAD_DIM = 64
NORM_EPS = 1e-6


def setup_inputs(seed: int = 0, part: int = 0) -> dict:
    root_key = jax.random.key(seed)
    k_act, k_norm, k_key, k_val = jax.random.split(root_key, 4)
    k_act = jax.random.fold_in(k_act, part)
    w_scale = D_MODEL ** -0.5
    w_shape = (N_LAYERS, D_MODEL, N_HEADS, HEAD_DIM)
    enc_out = jax.random.normal(k_act, (BATCH_SIZE, SEQ_LEN, D_MODEL), jnp.float32)
    norm_scale = jax.random.uniform(k_norm, (D_MODEL,), jnp.float32, 0.5, 1.5)
    w_key = jax.random.normal(k_key, w_shape, jnp.float32) * w_scale
    w_value = jax.random.normal(k_val, w_shape, jnp.float32) * w_scale
    return {"enc_out": enc_out.astype(jnp.bfloat16), "norm_scale": norm_scale.astype(jnp.bfloat16), "w_key": w_key.astype(jnp.bfloat16), "w_value": w_value.astype(jnp.bfloat16)}


def rms_norm(enc_out, norm_scale):
    acts = enc_out.astype(jnp.float32)
    mean_sq = jnp.mean(acts * acts, axis=-1, keepdims=True)
    return (acts * lax.rsqrt(mean_sq + NORM_EPS) * norm_scale.astype(jnp.float32)).astype(jnp.bfloat16)


def reference(enc_out, norm_scale, w_key, w_value):
    normed = rms_norm(enc_out, norm_scale).reshape(BATCH_SIZE * SEQ_LEN, D_MODEL)
    out_shape = (BATCH_SIZE, SEQ_LEN, N_HEADS, HEAD_DIM)

    def project(layer_weights):
        layer_key, layer_value = layer_weights
        keys = jnp.dot(normed, layer_key.reshape(D_MODEL, N_HEADS * HEAD_DIM), preferred_element_type=jnp.float32)
        values = jnp.dot(normed, layer_value.reshape(D_MODEL, N_HEADS * HEAD_DIM), preferred_element_type=jnp.float32)
        return keys.astype(jnp.bfloat16).reshape(out_shape), values.astype(jnp.bfloat16).reshape(out_shape)

    key_cache, value_cache = lax.map(project, (w_key, w_value))
    return key_cache, value_cache
```

```python
import functools

import jax
import jax.numpy as jnp
from jax import lax
from jax.experimental import pallas as pl
from jax.experimental.pallas import tpu as pltpu
from jax.sharding import PartitionSpec as P


NORM_EPS = 1e-6
MIB = 1024 * 1024
N_FLOPS = 8
ANY, VMEM = (pl.BlockSpec(memory_space=space) for space in (pl.ANY, pltpu.VMEM))

ORDER = (
    "n0", "m0", "n1", "m1", "m2", "sp0", "sp1", "sp2", "n_0", "n_1", "n_2",
    ("p0", "p1", "p2"),
    "fm0", "sm0",
    ("sp0", "sp1", "sp2", "m0"),
    "sn0", "fm1", "sm1",
    ("sm0", "n_0", "m1"),
    "sn1",
    ("sn0", "sm1", "n_1"),
    "fm2", "sm2",
    ("sn1", "m2"),
    "sn2",
    ("sm2", "n_2"),
    "sfm0",
    ("sn2", "fm0"),
    "sfm1",
    ("sfm0", "fm1"),
    ("sfm1",),
    "sfm2",
    ("fm2",),
    ("sfm2",),
)


def source(name):
    if name[0] == "s":
        inner = name[1:]
        return "n_" + inner[1:] if inner[0] == "n" else inner
    return name[1:] if name[0] == "f" else "p" + name[-1]


def norm(x, scale):
    acts = x.astype(jnp.float32)
    mean_sq = jnp.mean(acts * acts, axis=-1, keepdims=True)
    return (acts * lax.rsqrt(mean_sq + NORM_EPS) * scale).astype(jnp.bfloat16)


def norm_kernel(first, n_w, x_ref, scale_ref, *refs):
    weights = [pltpu.make_async_copy(refs[i], refs[-1 - n_w + i], refs[-1].at[i]) for i in range(n_w)]
    for copy in weights:
        copy.start()
    scale = scale_ref[...].astype(jnp.float32).reshape(1, -1)
    for out_ref in refs[n_w:len(refs) - 1 - n_w]:
        count = out_ref.shape[0]
        for b in range(count):
            out_ref[b] = norm(x_ref[first + b], scale)
        first += count
    for copy in weights:
        copy.wait()


def norm_pieces(enc_out, norm_scale, first, counts, weights):
    tokens, depth = enc_out.shape[1:]
    work = sum(counts) * tokens * depth
    return pl.pallas_call(
        functools.partial(norm_kernel, first, len(weights)),
        in_specs=[VMEM, VMEM] + [ANY] * len(weights),
        out_specs=[VMEM] * (len(counts) + len(weights)),
        out_shape=[jax.ShapeDtypeStruct((count, tokens, depth), jnp.bfloat16) for count in counts] + [jax.ShapeDtypeStruct(w.shape, w.dtype) for w in weights],
        scratch_shapes=[pltpu.SemaphoreType.DMA((2,))],
        compiler_params=pltpu.CompilerParams(vmem_limit_bytes=5 * MIB),
        cost_estimate=pl.CostEstimate(flops=work * N_FLOPS, bytes_accessed=work * 4, transcendentals=0),
    )(enc_out, norm_scale, *weights)


def project_kernel(pieces, group, slot0, before, last, *refs):
    n_x = len(pieces)
    x_refs, (wk_ref, wv_ref) = refs[:n_x], refs[n_x:n_x + 2]
    k_ref, v_ref, o_buf, _, _, x_buf, x_sem, o_sem = refs[-8:]
    layers, heads = k_ref.shape[0], k_ref.shape[2]
    tokens, depth = x_refs[0].shape[1:]
    me = lax.axis_index("tp")
    n_tp = lax.axis_size("tp")
    starts = [sum(rows for rows, _, _, _ in pieces[:p]) for p in range(n_x)]
    steps = sum(rows for rows, _, _, _ in pieces) // group
    far = [p for p in range(n_x) if pieces[p][3]]

    def x_copy(p):
        return pltpu.make_async_copy(x_refs[p], x_buf.at[pl.ds(starts[p], pieces[p][0])], x_sem.at[p])

    for p in far:
        x_copy(p).start()

    def owner_of(hop, flip):
        odd = lax.rem(me, 2)
        base = me + flip * (1 - 2 * odd)
        return lax.rem(base + 2 * hop * (2 * lax.rem(base, 2) - 1) + 2 * n_tp, n_tp)

    def place(block):
        seq = jnp.int32(0)
        owner = jnp.int32(0)
        for start, (rows, first, whose, _) in zip(starts, pieces):
            inside = block >= start
            seq = jnp.where(inside, first + block - start, seq)
            owner = jnp.where(inside, owner_of(*whose), owner)
        return seq, owner

    def o_copy(slot, w, g, seq, owner, results=o_buf):
        lanes = pl.ds(pl.multiple_of(owner * tokens, tokens), tokens)
        return pltpu.make_async_copy(results.at[slot, g, w], (k_ref, v_ref)[w].at[:, seq, :, lanes], o_sem.at[slot, g, w])

    def send(slot, where):
        for g, (seq, owner) in enumerate(where):
            for w in range(2):
                o_copy(slot, w, g, seq, owner).start()

    def wait(slot, count):
        for g in range(count):
            for w in range(2):
                o_copy(slot, w, g, 0, 0).wait()

    if before:
        for g, (seq, whose) in enumerate(before):
            for w in range(2):
                o_copy((slot0 + 1) % 2, w, g, seq, owner_of(*whose), refs[n_x + 4]).start()

    def step(s, carry):
        slot = lax.rem(s + slot0, 2)
        if before and steps > 1:
            @pl.when(s == 1)
            def _():
                wait((slot0 + 1) % 2, len(before))
        if steps > 2:
            @pl.when(s >= 2)
            def _():
                wait(slot, group)

        if n_x == 1 and not far:
            x = x_refs[0][pl.ds(group * s, group)]
        else:
            for p, x_ref in enumerate(x_refs):
                rows = pl.ds(starts[p], pieces[p][0])

                @pl.when(s == starts[p] // group)
                def _(p=p, x_ref=x_ref, rows=rows):
                    if p in far:
                        x_copy(p).wait()
                    else:
                        x_buf[rows] = x_ref[...]
            x = x_buf[pl.ds(group * s, group)]
        x = x.reshape(group * tokens, depth)
        chunk = 4
        for w, w_ref in enumerate((wk_ref, wv_ref)):
            for layer in range(0, layers, chunk):
                rows = w_ref[layer * heads:(layer + chunk) * heads, :]
                acc = lax.dot_general(rows, x, (((1,), (1,)), ((), ())), preferred_element_type=jnp.float32)
                acc = acc.astype(jnp.bfloat16).reshape(chunk, heads, group * tokens)
                for g in range(group):
                    o_buf[slot, g, w, layer:layer + chunk] = acc[:, :, g * tokens:(g + 1) * tokens]

        where = [place(group * s + g) for g in range(group)]
        if last:
            send(slot, where)
        elif steps > 1:
            @pl.when(s < steps - 1)
            def _():
                send(slot, where)
        return carry

    if steps == 1:
        step(0, 0)
    else:
        lax.fori_loop(0, steps, step, 0)
    if steps > 1:
        wait((slot0 + steps) % 2, group)
    elif before:
        wait((slot0 + 1) % 2, len(before))
    if last:
        wait((slot0 + steps - 1) % 2, group)


def project(pieces, state, shapes, slot0, before, last):
    cache, hold = shapes
    arrays = [piece[0] for piece in pieces]
    layout = [(x.shape[0], seq, whose, far) for x, seq, whose, far in pieces]
    total = sum(x.shape[0] for x in arrays)
    group = 4 if total >= 8 else 2
    tokens, depth = arrays[0].shape[1:]
    old, weights = state[:-2], state[-2:]
    operands = [*arrays, *weights, *old]
    n_x = len(arrays)
    aliases = {n_x: 3, n_x + 1: 4}
    if old:
        aliases.update({n_x + 2 + i: i for i in range(3)})
    staged = total if n_x > 1 or layout[0][3] else 1
    state = pl.pallas_call(
        functools.partial(project_kernel, layout, group, slot0, before, last),
        in_specs=[ANY if far else VMEM for _, _, _, far in layout] + [VMEM] * 2 + [ANY, ANY, VMEM][:len(old)],
        out_specs=[ANY, ANY, VMEM, VMEM, VMEM],
        out_shape=[cache, cache, hold, *(jax.ShapeDtypeStruct(w.shape, w.dtype) for w in weights)],
        input_output_aliases=aliases,
        scratch_shapes=[pltpu.VMEM((staged, tokens, depth), jnp.bfloat16), pltpu.SemaphoreType.DMA((n_x,)), pltpu.SemaphoreType.DMA((2, 4, 2))],
        compiler_params=pltpu.CompilerParams(vmem_limit_bytes=6 * MIB),
        cost_estimate=pl.CostEstimate(flops=total * tokens * depth, bytes_accessed=total * tokens * depth, transcendentals=0),
    )(*operands)
    blocks = [(first + r, whose) for rows, first, whose, _ in layout for r in range(rows)]
    return state, (slot0 + total // group) % 2, blocks[-group:]


def solution(mesh):
    n_tp = mesh.shape["tp"]
    perms = {
        "m": [(t, (t + 2 - 4 * (t % 2)) % n_tp) for t in range(n_tp)],
        "n": [(t, (t - 2 + 4 * (t % 2)) % n_tp) for t in range(n_tp)],
        "s": [(t, t ^ 1) for t in range(n_tp)],
    }
    hops = {"m": 1, "n": -1, "s": 0}

    def body(enc_out, norm_scale, w_key, w_value):
        layers, depth, n_heads, head_dim = w_key.shape
        n_seqs, tokens, _ = enc_out.shape
        heads = n_heads * head_dim
        third = n_seqs // 3
        wk = w_key.transpose(0, 2, 3, 1).reshape(layers * heads, depth)
        wv = w_value.transpose(0, 2, 3, 1).reshape(layers * heads, depth)
        cache = jax.ShapeDtypeStruct((layers, n_seqs, heads, tokens * n_tp), jnp.bfloat16)
        hold = jax.ShapeDtypeStruct((2, 4, 2, layers, heads, tokens), jnp.bfloat16)

        pieces = {}
        home = (0, 0)
        weights = state = before = None
        slot = 0
        for i, op in enumerate(ORDER):
            if op in ("n0", "n1"):
                count = 1 + int(op[-1])
                done = len(pieces) and 1
                made = norm_pieces(enc_out, norm_scale, third * done, [third] * count, (wk, wv) if done else ())
                if done:
                    *made, w_key, w_value = made
                    weights = (w_key, w_value)
                for part, x in enumerate(made, done):
                    pieces[f"p{part}"] = (x, third * part, home, False)
            elif isinstance(op, tuple):
                last = i == len(ORDER) - 1
                state, slot, before = project([pieces[name] for name in op], state or weights, (cache, hold), slot, before, last)
            else:
                way = "m" if op[0] == "f" else op[0]
                x, seq, (hop, flip), _ = pieces[source(op)]
                x = lax.ppermute(x, "tp", perms[way])
                pieces[op] = (x, seq, (hop + hops[way], flip + (way == "s")), way != "s")

        def leave(out):
            return out.reshape(layers, n_seqs, n_heads, head_dim, tokens * n_tp).transpose(0, 1, 4, 2, 3)

        return leave(state[0]), leave(state[1])

    weight_spec = P(None, None, "tp", None)
    cache_spec = P(None, "dp", None, "tp", None)
    return jax.shard_map(body, mesh=mesh, in_specs=(P("dp", "tp", None), P(None), weight_spec, weight_spec), out_specs=(cache_spec, cache_spec), check_vma=False)
```

```python
import functools

import jax
import jax.numpy as jnp
from jax import lax
from jax.experimental import pallas as pl
from jax.experimental.pallas import tpu as pltpu
from jax.sharding import PartitionSpec as P


NORM_EPS = 1e-6
MIB = 1024 * 1024
N_FLOPS = 8
PARTS = (4, 4, 4)
ANY, VMEM, HBM = (pl.BlockSpec(memory_space=space) for space in (pl.ANY, pltpu.VMEM, pltpu.HBM))

ORDER = (
    "n0",
    "m0",
    "n1",
    "m1",
    "m2",
    "sp0",
    "sp1",
    "sp2",
    "n_0",
    "n_1",
    "n_2",
    ("p0", "p1", "p2"),
    "fm0",
    "sm0",
    ("sp0", "sp1", "sp2", "m0"),
    "sn0",
    ("sm0", "n_0"),
    "fm1",
    "sm1",
    ("sn0", "m1"),
    "sn1",
    ("sm1", "n_1"),
    "fm2",
    "sm2",
    ("sn1", "m2", "sm2"),
    "sn2",
    ("n_2",),
    "sfm0",
    ("sn2", "fm0"),
    "sfm1",
    ("sfm0", "fm1"),
    ("sfm1",),
    "sfm2",
    ("fm2",),
    ("sfm2",),
)


def source(name):
    if name[0] == "s":
        inner = name[1:]
        return "n_" + inner[1:] if inner[0] == "n" else inner
    return name[1:] if name[0] == "f" else "p" + name[-1]


def norm(x, scale):
    acts = x.astype(jnp.float32)
    mean_sq = jnp.mean(acts * acts, axis=-1, keepdims=True)
    return (acts * lax.rsqrt(mean_sq + NORM_EPS) * scale).astype(jnp.bfloat16)


def norm_kernel(first, n_w, x_ref, scale_ref, *refs):
    outs = refs[n_w:-4 - n_w]
    x_buf, scale_buf, sem, w_sem = refs[-4:]
    total = sum(out_ref.shape[0] for out_ref in outs)
    copies = [pltpu.make_async_copy(x_ref.at[first + b], x_buf.at[b], sem.at[b]) for b in range(total)]
    scale_copy = pltpu.make_async_copy(scale_ref, scale_buf, sem.at[total])
    weights = [pltpu.make_async_copy(refs[i], refs[-4 - n_w + i], w_sem.at[i]) for i in range(n_w)]
    for copy in (scale_copy, *copies, *weights):
        copy.start()
    scale_copy.wait()
    scale = scale_buf[...].astype(jnp.float32).reshape(1, -1)
    at = 0
    for out_ref in outs:
        for b in range(out_ref.shape[0]):
            copies[at].wait()
            out_ref[b] = norm(x_buf[at], scale)
            at += 1
    for copy in weights:
        copy.wait()


def norm_pieces(enc_out, norm_scale, first, counts, weights):
    tokens, depth = enc_out.shape[1:]
    work = sum(counts) * tokens * depth
    return pl.pallas_call(
        functools.partial(norm_kernel, first, len(weights)),
        in_specs=[HBM] * (2 + len(weights)),
        out_specs=[VMEM] * (len(counts) + len(weights)),
        out_shape=[jax.ShapeDtypeStruct((count, tokens, depth), jnp.bfloat16) for count in counts] + [jax.ShapeDtypeStruct(w.shape, w.dtype) for w in weights],
        scratch_shapes=[pltpu.VMEM((sum(counts), tokens, depth), jnp.bfloat16), pltpu.VMEM((depth,), jnp.bfloat16), pltpu.SemaphoreType.DMA((sum(counts) + 1,)), pltpu.SemaphoreType.DMA((2,))],
        compiler_params=pltpu.CompilerParams(vmem_limit_bytes=8 * MIB),
        cost_estimate=pl.CostEstimate(flops=work * N_FLOPS, bytes_accessed=work * 4, transcendentals=0),
    )(*(pltpu.with_memory_space_constraint(x, pltpu.HBM) for x in (enc_out, norm_scale, *weights)))


def project_kernel(pieces, group, slot0, before, last, *refs):
    n_x = len(pieces)
    x_refs, (wk_ref, wv_ref) = refs[:n_x], refs[n_x:n_x + 2]
    k_ref, v_ref, o_buf, _, _, x_buf, x_sem, o_sem = refs[-8:]
    layers, heads = k_ref.shape[0], k_ref.shape[2]
    tokens, depth = x_refs[0].shape[1:]
    me = lax.axis_index("tp")
    n_tp = lax.axis_size("tp")
    starts = [sum(rows for rows, _, _, _ in pieces[:p]) for p in range(n_x)]
    steps = sum(rows for rows, _, _, _ in pieces) // group
    far = [p for p in range(n_x) if pieces[p][3]]

    def x_copy(p):
        return pltpu.make_async_copy(x_refs[p], x_buf.at[pl.ds(starts[p], pieces[p][0])], x_sem.at[p])

    for p in far:
        x_copy(p).start()

    def owner_of(hop, flip):
        odd = lax.rem(me, 2)
        base = me + flip * (1 - 2 * odd)
        return lax.rem(base + 2 * hop * (2 * lax.rem(base, 2) - 1) + 2 * n_tp, n_tp)

    def place(block):
        seq = jnp.int32(0)
        owner = jnp.int32(0)
        for start, (rows, first, whose, _) in zip(starts, pieces):
            inside = block >= start
            seq = jnp.where(inside, first + block - start, seq)
            owner = jnp.where(inside, owner_of(*whose), owner)
        return seq, owner

    def o_copy(slot, w, g, seq, owner, results=o_buf):
        lanes = pl.ds(pl.multiple_of(owner * tokens, tokens), tokens)
        return pltpu.make_async_copy(results.at[slot, g, w], (k_ref, v_ref)[w].at[:, seq, :, lanes], o_sem.at[slot, g, w])

    def send(slot, where):
        for g, (seq, owner) in enumerate(where):
            for w in range(2):
                o_copy(slot, w, g, seq, owner).start()

    def wait(slot, count):
        for g in range(count):
            for w in range(2):
                o_copy(slot, w, g, 0, 0).wait()

    if before:
        for g, (seq, whose) in enumerate(before):
            for w in range(2):
                o_copy((slot0 + 1) % 2, w, g, seq, owner_of(*whose), refs[n_x + 4]).start()

    def step(s, carry):
        slot = lax.rem(s + slot0, 2)
        if before and steps > 1:
            @pl.when(s == 1)
            def _():
                wait((slot0 + 1) % 2, len(before))
        if steps > 2:
            @pl.when(s >= 2)
            def _():
                wait(slot, group)

        if n_x == 1 and not far:
            x = x_refs[0][pl.ds(group * s, group)]
        else:
            for p, x_ref in enumerate(x_refs):
                rows = pl.ds(starts[p], pieces[p][0])

                @pl.when(s == starts[p] // group)
                def _(p=p, x_ref=x_ref, rows=rows):
                    if p in far:
                        x_copy(p).wait()
                    else:
                        x_buf[rows] = x_ref[...]
            x = x_buf[pl.ds(group * s, group)]
        x = x.reshape(group * tokens, depth)
        chunk = 4
        for w, w_ref in enumerate((wk_ref, wv_ref)):
            for layer in range(0, layers, chunk):
                rows = w_ref[layer * heads:(layer + chunk) * heads, :]
                acc = lax.dot_general(rows, x, (((1,), (1,)), ((), ())), preferred_element_type=jnp.float32)
                acc = acc.astype(jnp.bfloat16).reshape(chunk, heads, group * tokens)
                for g in range(group):
                    o_buf[slot, g, w, layer:layer + chunk] = acc[:, :, g * tokens:(g + 1) * tokens]

        where = [place(group * s + g) for g in range(group)]
        if last:
            send(slot, where)
        elif steps > 1:
            @pl.when(s < steps - 1)
            def _():
                send(slot, where)
        return carry

    if steps == 1:
        step(0, 0)
    else:
        lax.fori_loop(0, steps, step, 0)
    if steps > 1:
        wait((slot0 + steps) % 2, group)
    elif before:
        wait((slot0 + 1) % 2, len(before))
    if last:
        wait((slot0 + steps - 1) % 2, group)


def project(pieces, state, shapes, slot0, before, last):
    cache, hold = shapes
    arrays = [piece[0] for piece in pieces]
    layout = [(x.shape[0], seq, whose, far) for x, seq, whose, far in pieces]
    total = sum(x.shape[0] for x in arrays)
    group = 4 if total >= 8 and total % 4 == 0 else 2
    tokens, depth = arrays[0].shape[1:]
    old, weights = state[:-2], state[-2:]
    operands = [*arrays, *weights, *old]
    n_x = len(arrays)
    aliases = {n_x: 3, n_x + 1: 4}
    if old:
        aliases.update({n_x + 2 + i: i for i in range(3)})
    staged = total if n_x > 1 or layout[0][3] else 1
    state = pl.pallas_call(
        functools.partial(project_kernel, layout, group, slot0, before, last),
        in_specs=[ANY if far else VMEM for _, _, _, far in layout] + [VMEM] * 2 + [ANY, ANY, VMEM][:len(old)],
        out_specs=[ANY, ANY, VMEM, VMEM, VMEM],
        out_shape=[cache, cache, hold, *(jax.ShapeDtypeStruct(w.shape, w.dtype) for w in weights)],
        input_output_aliases=aliases,
        scratch_shapes=[pltpu.VMEM((staged, tokens, depth), jnp.bfloat16), pltpu.SemaphoreType.DMA((n_x,)), pltpu.SemaphoreType.DMA((2, 4, 2))],
        compiler_params=pltpu.CompilerParams(vmem_limit_bytes=6 * MIB),
        cost_estimate=pl.CostEstimate(flops=total * tokens * depth, bytes_accessed=total * tokens * depth, transcendentals=0),
    )(*operands)
    blocks = [(first + r, whose) for rows, first, whose, _ in layout for r in range(rows)]
    return state, (slot0 + total // group) % 2, blocks[-group:]


def solution(mesh):
    n_tp = mesh.shape["tp"]
    perms = {
        "m": [(t, (t + 2 - 4 * (t % 2)) % n_tp) for t in range(n_tp)],
        "n": [(t, (t - 2 + 4 * (t % 2)) % n_tp) for t in range(n_tp)],
        "s": [(t, t ^ 1) for t in range(n_tp)],
    }
    hops = {"m": 1, "n": -1, "s": 0}

    def body(enc_out, norm_scale, w_key, w_value):
        layers, depth, n_heads, head_dim = w_key.shape
        n_seqs, tokens, _ = enc_out.shape
        heads = n_heads * head_dim
        sizes = [n_seqs * part // 12 for part in PARTS]
        firsts = [sum(sizes[:part]) for part in range(len(sizes))]
        wk = w_key.transpose(0, 2, 3, 1).reshape(layers * heads, depth)
        wv = w_value.transpose(0, 2, 3, 1).reshape(layers * heads, depth)
        cache = jax.ShapeDtypeStruct((layers, n_seqs, heads, tokens * n_tp), jnp.bfloat16)
        hold = jax.ShapeDtypeStruct((2, 4, 2, layers, heads, tokens), jnp.bfloat16)

        pieces = {}
        home = (0, 0)
        weights = state = before = None
        slot = 0
        for i, op in enumerate(ORDER):
            if op in ("n0", "n1"):
                done = int(op[-1])
                counts = sizes[1:] if done else sizes[:1]
                made = norm_pieces(enc_out, norm_scale, firsts[done], counts, (wk, wv) if done else ())
                if done:
                    *made, w_key, w_value = made
                    weights = (w_key, w_value)
                for part, x in enumerate(made, done):
                    pieces[f"p{part}"] = (x, firsts[part], home, False)
            elif isinstance(op, tuple):
                last = i == len(ORDER) - 1
                state, slot, before = project([pieces[name] for name in op], state or weights, (cache, hold), slot, before, last)
            else:
                way = "m" if op[0] == "f" else op[0]
                x, seq, (hop, flip), _ = pieces[source(op)]
                x = lax.ppermute(x, "tp", perms[way])
                pieces[op] = (x, seq, (hop + hops[way], flip + (way == "s")), way != "s")

        def leave(out):
            return out.reshape(layers, n_seqs, n_heads, head_dim, tokens * n_tp).transpose(0, 1, 4, 2, 3)

        return leave(state[0]), leave(state[1])

    weight_spec = P(None, None, "tp", None)
    cache_spec = P(None, "dp", None, "tp", None)
    return jax.shard_map(body, mesh=mesh, in_specs=(P("dp", "tp", None), P(None), weight_spec, weight_spec), out_specs=(cache_spec, cache_spec), check_vma=False)
```

```python
import functools

import jax
import jax.numpy as jnp
from jax import lax
from jax.experimental import pallas as pl
from jax.experimental.pallas import tpu as pltpu
from jax.sharding import PartitionSpec as P


NORM_EPS = 1e-6
MIB = 1024 * 1024
N_FLOPS = 8
PARTS = (4, 4, 4)
ANY, VMEM, HBM = (pl.BlockSpec(memory_space=space) for space in (pl.ANY, pltpu.VMEM, pltpu.HBM))

ORDER = (
    "n0",
    "m0",
    "n1",
    "m1",
    "m2",
    "sp0",
    "sp1",
    "sp2",
    "n_0",
    "n_1",
    "n_2",
    ("p0", "p1", "p2"),
    "fm0",
    "sm0",
    ("sp0", "sp1", "sp2", "m0"),
    "sn0",
    ("sm0", "n_0"),
    "fm1",
    "sm1",
    ("sn0", "m1"),
    "sn1",
    ("sm1", "n_1"),
    "fm2",
    "sm2",
    ("sn1", "m2", "sm2"),
    "sn2",
    ("n_2",),
    "sfm0",
    ("sn2", "fm0"),
    "sfm1",
    ("sfm0", "fm1"),
    ("sfm1",),
    "sfm2",
    ("fm2",),
    ("sfm2",),
)


def source(name):
    if name[0] == "s":
        inner = name[1:]
        return "n_" + inner[1:] if inner[0] == "n" else inner
    return name[1:] if name[0] == "f" else "p" + name[-1]


def norm(x, scale):
    acts = x.astype(jnp.float32)
    mean_sq = jnp.mean(acts * acts, axis=-1, keepdims=True)
    return (acts * lax.rsqrt(mean_sq + NORM_EPS) * scale).astype(jnp.bfloat16)


def norm_kernel(first, n_w, x_ref, scale_ref, *refs):
    outs = refs[n_w:-4 - n_w]
    x_buf, scale_buf, sem, w_sem = refs[-4:]
    total = sum(out_ref.shape[0] for out_ref in outs)
    copies = [pltpu.make_async_copy(x_ref.at[first + b], x_buf.at[b], sem.at[b]) for b in range(total)]
    scale_copy = pltpu.make_async_copy(scale_ref, scale_buf, sem.at[total])
    weights = [pltpu.make_async_copy(refs[i], refs[-4 - n_w + i], w_sem.at[i]) for i in range(n_w)]
    for copy in (scale_copy, *copies, *weights):
        copy.start()
    scale_copy.wait()
    scale = scale_buf[...].astype(jnp.float32).reshape(1, -1)
    at = 0
    for out_ref in outs:
        for b in range(out_ref.shape[0]):
            copies[at].wait()
            out_ref[b] = norm(x_buf[at], scale)
            at += 1
    for copy in weights:
        copy.wait()


def norm_pieces(enc_out, norm_scale, first, counts, weights):
    tokens, depth = enc_out.shape[1:]
    work = sum(counts) * tokens * depth
    return pl.pallas_call(
        functools.partial(norm_kernel, first, len(weights)),
        in_specs=[HBM] * (2 + len(weights)),
        out_specs=[VMEM] * (len(counts) + len(weights)),
        out_shape=[jax.ShapeDtypeStruct((count, tokens, depth), jnp.bfloat16) for count in counts] + [jax.ShapeDtypeStruct(w.shape, w.dtype) for w in weights],
        scratch_shapes=[pltpu.VMEM((sum(counts), tokens, depth), jnp.bfloat16), pltpu.VMEM((depth,), jnp.bfloat16), pltpu.SemaphoreType.DMA((sum(counts) + 1,)), pltpu.SemaphoreType.DMA((2,))],
        compiler_params=pltpu.CompilerParams(vmem_limit_bytes=8 * MIB),
        cost_estimate=pl.CostEstimate(flops=work * N_FLOPS, bytes_accessed=work * 4, transcendentals=0),
    )(*(pltpu.with_memory_space_constraint(x, pltpu.HBM) for x in (enc_out, norm_scale, *weights)))


def project_kernel(pieces, group, slot0, before, last, *refs):
    n_x = len(pieces)
    x_refs, (wk_ref, wv_ref) = refs[:n_x], refs[n_x:n_x + 2]
    k_ref, v_ref, o_buf, _, wv_held, x_buf, x_sem, o_sem, w_sem = refs[-9:]
    layers, heads = k_ref.shape[0], k_ref.shape[2]
    tokens, depth = x_refs[0].shape[1:]
    me = lax.axis_index("tp")
    n_tp = lax.axis_size("tp")
    starts = [sum(rows for rows, _, _, _ in pieces[:p]) for p in range(n_x)]
    steps = sum(rows for rows, _, _, _ in pieces) // group
    far = [p for p in range(n_x) if pieces[p][3]]

    def x_copy(p):
        return pltpu.make_async_copy(x_refs[p], x_buf.at[pl.ds(starts[p], pieces[p][0])], x_sem.at[p])

    load = None if before else pltpu.make_async_copy(wv_ref, wv_held, w_sem)
    if load:
        load.start()
        wv_ref = wv_held
    for p in far:
        x_copy(p).start()

    def owner_of(hop, flip):
        odd = lax.rem(me, 2)
        base = me + flip * (1 - 2 * odd)
        return lax.rem(base + 2 * hop * (2 * lax.rem(base, 2) - 1) + 2 * n_tp, n_tp)

    def place(block):
        seq = jnp.int32(0)
        owner = jnp.int32(0)
        for start, (rows, first, whose, _) in zip(starts, pieces):
            inside = block >= start
            seq = jnp.where(inside, first + block - start, seq)
            owner = jnp.where(inside, owner_of(*whose), owner)
        return seq, owner

    def o_copy(slot, w, g, seq, owner, results=o_buf):
        lanes = pl.ds(pl.multiple_of(owner * tokens, tokens), tokens)
        return pltpu.make_async_copy(results.at[slot, g, w], (k_ref, v_ref)[w].at[:, seq, :, lanes], o_sem.at[slot, g, w])

    def send(slot, where):
        for g, (seq, owner) in enumerate(where):
            for w in range(2):
                o_copy(slot, w, g, seq, owner).start()

    def wait(slot, count):
        for g in range(count):
            for w in range(2):
                o_copy(slot, w, g, 0, 0).wait()

    if before:
        for g, (seq, whose) in enumerate(before):
            for w in range(2):
                o_copy((slot0 + 1) % 2, w, g, seq, owner_of(*whose), refs[n_x + 4]).start()

    def step(s, carry):
        slot = lax.rem(s + slot0, 2)
        if before and steps > 1:
            @pl.when(s == 1)
            def _():
                wait((slot0 + 1) % 2, len(before))
        if steps > 2:
            @pl.when(s >= 2)
            def _():
                wait(slot, group)

        if n_x == 1 and not far:
            x = x_refs[0][pl.ds(group * s, group)]
        else:
            for p, x_ref in enumerate(x_refs):
                rows = pl.ds(starts[p], pieces[p][0])

                @pl.when(s == starts[p] // group)
                def _(p=p, x_ref=x_ref, rows=rows):
                    if p in far:
                        x_copy(p).wait()
                    else:
                        x_buf[rows] = x_ref[...]
            x = x_buf[pl.ds(group * s, group)]
        x = x.reshape(group * tokens, depth)
        chunk = 4
        for w, w_ref in enumerate((wk_ref, wv_ref)):
            if w and load:
                @pl.when(s == 0)
                def _():
                    load.wait()
            for layer in range(0, layers, chunk):
                rows = w_ref[layer * heads:(layer + chunk) * heads, :]
                acc = lax.dot_general(rows, x, (((1,), (1,)), ((), ())), preferred_element_type=jnp.float32)
                acc = acc.astype(jnp.bfloat16).reshape(chunk, heads, group * tokens)
                for g in range(group):
                    o_buf[slot, g, w, layer:layer + chunk] = acc[:, :, g * tokens:(g + 1) * tokens]

        where = [place(group * s + g) for g in range(group)]
        if last:
            send(slot, where)
        elif steps > 1:
            @pl.when(s < steps - 1)
            def _():
                send(slot, where)
        return carry

    if steps == 1:
        step(0, 0)
    else:
        lax.fori_loop(0, steps, step, 0)
    if steps > 1:
        wait((slot0 + steps) % 2, group)
    elif before:
        wait((slot0 + 1) % 2, len(before))
    if last:
        wait((slot0 + steps - 1) % 2, group)


def project(pieces, state, shapes, slot0, before, last):
    cache, hold = shapes
    arrays = [piece[0] for piece in pieces]
    layout = [(x.shape[0], seq, whose, far) for x, seq, whose, far in pieces]
    total = sum(x.shape[0] for x in arrays)
    group = 4 if total >= 8 and total % 4 == 0 else 2
    tokens, depth = arrays[0].shape[1:]
    old, weights = state[:-2], state[-2:]
    operands = [*arrays, *weights, *old]
    n_x = len(arrays)
    aliases = {n_x: 3}
    if old:
        aliases.update({n_x + 1: 4, **{n_x + 2 + i: i for i in range(3)}})
    else:
        operands[-1] = pltpu.with_memory_space_constraint(operands[-1], pltpu.HBM)
    staged = total if n_x > 1 or layout[0][3] else 1
    state = pl.pallas_call(
        functools.partial(project_kernel, layout, group, slot0, before, last),
        in_specs=[ANY if far else VMEM for _, _, _, far in layout] + [VMEM, VMEM if old else HBM] + [ANY, ANY, VMEM][:len(old)],
        out_specs=[ANY, ANY, VMEM, VMEM, VMEM],
        out_shape=[cache, cache, hold, *(jax.ShapeDtypeStruct(w.shape, w.dtype) for w in weights)],
        input_output_aliases=aliases,
        scratch_shapes=[pltpu.VMEM((staged, tokens, depth), jnp.bfloat16), pltpu.SemaphoreType.DMA((n_x,)), pltpu.SemaphoreType.DMA((2, 4, 2)), pltpu.SemaphoreType.DMA],
        compiler_params=pltpu.CompilerParams(vmem_limit_bytes=6 * MIB),
        cost_estimate=pl.CostEstimate(flops=total * tokens * depth, bytes_accessed=total * tokens * depth, transcendentals=0),
    )(*operands)
    blocks = [(first + r, whose) for rows, first, whose, _ in layout for r in range(rows)]
    return state, (slot0 + total // group) % 2, blocks[-group:]


def solution(mesh):
    n_tp = mesh.shape["tp"]
    perms = {
        "m": [(t, (t + 2 - 4 * (t % 2)) % n_tp) for t in range(n_tp)],
        "n": [(t, (t - 2 + 4 * (t % 2)) % n_tp) for t in range(n_tp)],
        "s": [(t, t ^ 1) for t in range(n_tp)],
    }
    hops = {"m": 1, "n": -1, "s": 0}

    def body(enc_out, norm_scale, w_key, w_value):
        layers, depth, n_heads, head_dim = w_key.shape
        n_seqs, tokens, _ = enc_out.shape
        heads = n_heads * head_dim
        sizes = [n_seqs * part // 12 for part in PARTS]
        firsts = [sum(sizes[:part]) for part in range(len(sizes))]
        wk = w_key.transpose(0, 2, 3, 1).reshape(layers * heads, depth)
        wv = w_value.transpose(0, 2, 3, 1).reshape(layers * heads, depth)
        cache = jax.ShapeDtypeStruct((layers, n_seqs, heads, tokens * n_tp), jnp.bfloat16)
        hold = jax.ShapeDtypeStruct((2, 4, 2, layers, heads, tokens), jnp.bfloat16)

        pieces = {}
        home = (0, 0)
        weights = state = before = None
        slot = 0
        for i, op in enumerate(ORDER):
            if op in ("n0", "n1"):
                done = int(op[-1])
                counts = sizes[1:] if done else sizes[:1]
                made = norm_pieces(enc_out, norm_scale, firsts[done], counts, (wk,) if done else ())
                if done:
                    *made, w_key = made
                    weights = (w_key, wv)
                for part, x in enumerate(made, done):
                    pieces[f"p{part}"] = (x, firsts[part], home, False)
            elif isinstance(op, tuple):
                last = i == len(ORDER) - 1
                state, slot, before = project([pieces[name] for name in op], state or weights, (cache, hold), slot, before, last)
            else:
                way = "m" if op[0] == "f" else op[0]
                x, seq, (hop, flip), _ = pieces[source(op)]
                x = lax.ppermute(x, "tp", perms[way])
                pieces[op] = (x, seq, (hop + hops[way], flip + (way == "s")), way != "s")

        def leave(out):
            return out.reshape(layers, n_seqs, n_heads, head_dim, tokens * n_tp).transpose(0, 1, 4, 2, 3)

        return leave(state[0]), leave(state[1])

    weight_spec = P(None, None, "tp", None)
    cache_spec = P(None, "dp", None, "tp", None)
    return jax.shard_map(body, mesh=mesh, in_specs=(P("dp", "tp", None), P(None), weight_spec, weight_spec), out_specs=(cache_spec, cache_spec), check_vma=False)
```
